32 devices in a mesh: dp: 4 (over x, core), expert: 8 (over z, y).
Axes of the slice: x: 2, y: 2, z: 4, core: 2. Of those that a mesh axis runs over, the one named last changes fastest.
Arguments:
- tokens: bfloat16 [5120, 131072], P(None, ('dp', 'expert')), may hold values from -24 to 24, as said below
- router: bfloat16 [5120, 40], P(None, 'expert'), may hold values from -1 to 1, as said below
- device_pick: int32 [3, 131072], P(None, 'dp'), may hold values from 0 to 7, as said below
- expert_pick: int32 [6, 131072], P(None, 'dp'), may hold values from 0 to 39, as said below
Outputs:
- gates: float32 [6, 131072], P(None, 'dp')
- device_max: float32 [8, 131072], P('expert', 'dp')
- balance: float32 [3], replicated
The draws below stay inside these ranges and needn't reach their ends.
Inputs may be any that keep to these rules, and one draw needn't show every extreme that they name: tokens lie within the range; in each column the values are of order one, except in a few columns. router entries are of order 1 / sqrt(5120). `device_pick`: each column names 3 different devices. `expert_pick`: each column names 6 different experts, two on each device of the column's device_pick, in that order; the device of expert e is e // 5.
All inputs are finite; a program needn't handle non-finite values.
Results may differ from the reference program's by a relative error of at most 0.0003.
Values may be sent and summed in bfloat16 or wider, within the bound.
A program may use at most 128 MiB of HBM per device.

```python
import jax
import jax.numpy as jnp
from jax import lax

D = 5120
EXP_DEV = 5
TOP = 6
DEV_TOP = 3
TOK_DEV = 32768
NDEV = 8
E = 40
TOKENS = 131072


def router_base(key):
    values = jax.random.normal(jax.random.fold_in(key, 7), (D, E), jnp.float32)
    return jnp.clip(values, -6.0, 6.0) * D ** (-0.5)


def draw_router(key, part):
    return router_base(key).astype(jnp.bfloat16)


def draw_tokens(key, part):
    inner = jax.random.fold_in(key, 3)
    shared = jax.random.normal(jax.random.fold_in(inner, 1), (D,), jnp.float32) * 0.5
    values = jax.random.normal(jax.random.fold_in(inner, 4), (TOKENS, D), jnp.float32) + shared[None, :]
    return jnp.clip(values, -24.0, 24.0).T.astype(jnp.bfloat16)


def draw_picks(key):
    inner = jax.random.fold_in(key, 11)
    span = max(TOK_DEV // 2, 1)
    blocks = (TOKENS + span - 1) // span
    hot_table = jax.random.randint(jax.random.fold_in(inner, 1), (blocks, 4), 0, NDEV)
    rows = jnp.arange(TOKENS, dtype=jnp.int32)
    hot_rows = hot_table[rows // span]
    slots = jnp.arange(NDEV, dtype=jnp.int32)
    hot = jnp.any(hot_rows[:, :, None] == slots[None, None, :], axis=1).astype(jnp.int32)
    noise = jax.random.randint(jax.random.fold_in(inner, 2), (TOKENS, NDEV), 0, 2 ** 22)
    keyed = (noise + hot * 2 ** 21) * NDEV + slots[None, :]
    _, chosen_dev = lax.top_k(keyed, DEV_TOP)
    chosen_dev = chosen_dev.astype(jnp.int32)
    local_noise = jax.random.randint(jax.random.fold_in(inner, 3), (TOKENS, DEV_TOP, EXP_DEV), 0, 2 ** 20)
    local_keyed = local_noise * EXP_DEV + jnp.arange(EXP_DEV, dtype=jnp.int32)[None, None, :]
    _, local_slot = lax.top_k(local_keyed, 2)
    experts = chosen_dev[:, :, None] * EXP_DEV + local_slot.astype(jnp.int32)
    return (chosen_dev.T, experts.reshape(TOKENS, TOP).T.astype(jnp.int32))


def draw_device_pick(key, part):
    return draw_picks(key)[0]


def draw_expert_pick(key, part):
    return draw_picks(key)[1]


def setup_inputs(seed: int = 0) -> dict:
    keys = jax.random.split(jax.random.key(seed), 5)
    tokens = draw_tokens(jax.random.fold_in(keys[4], 71), 0)
    router = draw_router(jax.random.fold_in(keys[4], 71), 0)
    device_pick = draw_device_pick(jax.random.fold_in(keys[4], 71), 0)
    expert_pick = draw_expert_pick(jax.random.fold_in(keys[4], 71), 0)
    return {"tokens": tokens, "router": router, "device_pick": device_pick, "expert_pick": expert_pick}


def reference(tokens, router, device_pick, expert_pick):
    scores = jnp.dot(router.T, tokens, preferred_element_type=jnp.float32)
    peak = jnp.max(scores, axis=0, keepdims=True)
    raised = jnp.exp(scores - peak)
    probs = raised / jnp.sum(raised, axis=0, keepdims=True)
    gates = jnp.take_along_axis(probs, expert_pick, axis=0)
    device_max = jnp.max(probs.reshape(NDEV, EXP_DEV, TOKENS), axis=1)
    ones_exp = jnp.ones((TOKENS * TOP,), jnp.float32)
    counts = jax.ops.segment_sum(ones_exp, expert_pick.reshape(-1), num_segments=E)
    ones_dev = jnp.ones((TOKENS * DEV_TOP,), jnp.float32)
    sent_counts = jax.ops.segment_sum(ones_dev, device_pick.reshape(-1), num_segments=NDEV)
    freq = counts * (E / (TOP * TOKENS))
    prob = jnp.sum(probs, axis=1) / TOKENS
    dev_freq = jnp.mean(freq.reshape(NDEV, EXP_DEV), axis=1)
    dev_prob = jnp.sum(prob.reshape(NDEV, EXP_DEV), axis=1)
    sent = sent_counts * (NDEV / (DEV_TOP * TOKENS))
    balance = jnp.stack([jnp.sum(freq * prob), jnp.sum(dev_freq * dev_prob), jnp.sum(sent * dev_prob)])
    return gates, device_max, balance
```

```python
import functools

import jax
import jax.numpy as jnp
from jax import lax
from jax.experimental import pallas as pl
from jax.experimental.pallas import tpu as pltpu
from jax.sharding import PartitionSpec as P

MESH = pl.DeviceIdType.MESH
TOP = 6
DEV_TOP = 3
SLOT = 8
LOG2E = 1.4426950408889634
GATE_SCALE = 2048.0
MAX_SCALE = 1048576.0
NEG = -1e30


def kernel(
    sizes, tokens, router, device_pick, expert_pick,
    gates, device_max, balance,
    tok, rows, picks, dpicks, sent_msg, recv_msg, cnt_msg, cnt_recv, bal_msg, bal_recv, prob_acc,
    tok_sem, pick_sem, rs_sem, rr_sem, ps_sem, pr_sem, ms_sem, mr_sem, cs_sem, cr_sem, bs_sem, br_sem,
):
    ndp, ndev, per_dev, width, chunks = sizes
    depth = tokens.shape[0]
    share = tokens.shape[1]
    total = share * ndev * ndp
    nrows = ndev * SLOT
    everyone = ndp * ndev
    half = depth // 2
    dp, me = lax.axis_index("dp"), lax.axis_index("expert")
    lin = dp * ndev + me
    core = lax.rem(dp, 2)
    partner = dp + 1 - 2 * core

    def token_copy(c):
        return pltpu.make_async_copy(
            tokens.at[:, pl.ds(pl.multiple_of(c * width, width), width)], tok.at[c], tok_sem.at[c]
        )

    mine = pl.ds(pl.multiple_of(me * share, share), share)
    pick_copy = pltpu.make_async_copy(expert_pick.at[:, mine], picks, pick_sem.at[0])
    dpick_copy = pltpu.make_async_copy(device_pick.at[:, mine], dpicks, pick_sem.at[1])
    pick_copy.start()
    dpick_copy.start()
    for c in range(chunks):
        token_copy(c).start()

    barrier = pltpu.get_barrier_semaphore()

    def other(j):
        t = lax.rem(lin + j, everyone)
        return (t // ndev, lax.rem(t, ndev))

    def greet(j, carry):
        pl.semaphore_signal(barrier, inc=1, device_id=other(j), device_id_type=MESH)
        return carry

    lax.fori_loop(1, everyone, greet, 0)
    pl.semaphore_wait(barrier, everyone - 1)

    my_half = pl.ds(pl.multiple_of(core * half, half), half)
    other_half = pl.ds(pl.multiple_of((1 - core) * half, half), half)
    my_rows = pl.ds(pl.multiple_of(me * SLOT, SLOT), SLOT)

    def router_copy(j):
        peer = lax.rem(me + j, ndev)
        return pltpu.make_async_remote_copy(
            src_ref=router.at[:, my_half], dst_ref=rows.at[my_rows, my_half],
            send_sem=rs_sem.at[j], recv_sem=rr_sem.at[j], device_id=(dp, peer), device_id_type=MESH,
        )

    def partner_copy(j):
        src = lax.rem(me + ndev - j, ndev)
        block = rows.at[pl.ds(pl.multiple_of(src * SLOT, SLOT), SLOT), my_half]
        return pltpu.make_async_remote_copy(
            src_ref=block, dst_ref=block, send_sem=ps_sem.at[j], recv_sem=pr_sem.at[j],
            device_id=(partner, me), device_id_type=MESH,
        )

    for j in range(1, ndev):
        router_copy(j).start()
    own = pltpu.make_async_copy(router, rows.at[my_rows, :], rs_sem.at[0])
    own.start()

    pick_copy.wait()
    dpick_copy.wait()
    row = lax.broadcasted_iota(jnp.int32, (nrows, 128), 0)
    lane = lax.broadcasted_iota(jnp.int32, (nrows, 128), 1)
    one, nil = jnp.float32(1.0), jnp.float32(0.0)
    ids = (row // SLOT) * per_dev + lax.rem(row, SLOT)
    ids = jnp.where(lax.rem(row, SLOT) < per_dev, ids, -1)
    dev_ids = jnp.where(lax.rem(row, SLOT) == 0, row // SLOT, -1)

    def count(i, carry):
        counts, sends = carry
        cols = pl.ds(pl.multiple_of(i * 128, 128), 128)
        for k in range(TOP):
            counts = counts + jnp.where(picks[k : k + 1, cols] == ids, one, nil)
        for k in range(DEV_TOP):
            sends = sends + jnp.where(dpicks[k : k + 1, cols] == dev_ids, one, nil)
        return counts, sends

    zero = jnp.zeros((nrows, 128), jnp.float32)
    counts, sends = lax.fori_loop(0, share // 128, count, (zero, zero))
    counts = jnp.sum(counts, axis=1, keepdims=True)
    sends = jnp.sum(sends, axis=1, keepdims=True)
    pages = cnt_msg.shape[1] // 2 // 128
    for p in range(pages):
        spot = row == lane + p * 128
        cnt_msg[:, p * 128 : (p + 1) * 128] = jnp.sum(jnp.where(spot, counts, nil), axis=0, keepdims=True)
        cnt_msg[:, (pages + p) * 128 : (pages + p + 1) * 128] = jnp.sum(
            jnp.where(spot, sends, nil), axis=0, keepdims=True
        )
    cnt_recv[lin] = cnt_msg[...]

    def count_copy(j):
        return pltpu.make_async_remote_copy(
            src_ref=cnt_msg, dst_ref=cnt_recv.at[lin], send_sem=cs_sem, recv_sem=cr_sem,
            device_id=other(j), device_id_type=MESH,
        )

    def start_count(j, carry):
        count_copy(j).start()
        return carry

    lax.fori_loop(1, everyone, start_count, 0)

    own.wait()
    for j in range(1, ndev):
        router_copy(j).wait_recv()
        partner_copy(j).start()
    for j in range(1, ndev):
        partner_copy(j).wait_recv()

    prob_acc[...] = zero
    wide_row = lax.broadcasted_iota(jnp.int32, (nrows, width), 0)
    wide_ids = (wide_row // SLOT) * per_dev + lax.rem(wide_row, SLOT)
    real = lax.rem(wide_row, SLOT) < per_dev
    wide_ids = jnp.where(real, wide_ids, -1)
    msg_row = lax.broadcasted_iota(jnp.int32, (4, width), 0)

    def message_copy(j, c):
        peer = lax.rem(me + j, ndev)
        return pltpu.make_async_remote_copy(
            src_ref=sent_msg.at[peer, c], dst_ref=recv_msg.at[me, c],
            send_sem=ms_sem.at[j], recv_sem=mr_sem.at[j], device_id=(dp, peer), device_id_type=MESH,
        )

    def step(c, carry):
        token_copy(c).wait()
        scores = jnp.dot(rows[...], tok[c], preferred_element_type=jnp.float32)
        scores = jnp.where(real, scores, NEG)
        peak = jnp.max(scores, axis=0, keepdims=True)
        shifted = scores - peak
        raised = jnp.exp(shifted)
        norm = jnp.sum(raised, axis=0, keepdims=True)
        probs = raised * (1.0 / norm)
        acc = prob_acc[...]
        for i in range(width // 128):
            acc = acc + probs[:, i * 128 : (i + 1) * 128]
        prob_acc[...] = acc
        log_norm = jnp.log(norm)
        cols = pl.ds(pl.multiple_of(c * width, width), width)
        codes = []
        for k in range(TOP):
            hit = picks[k : k + 1, cols] == wide_ids
            picked = jnp.sum(jnp.where(hit, shifted, nil), axis=0, keepdims=True)
            code = (log_norm - picked) * (LOG2E * GATE_SCALE) + 0.5
            codes.append(jnp.clip(code, 0.0, 65535.0).astype(jnp.int32))
        words = [codes[k] + jnp.left_shift(codes[k + TOP // 2], 16) for k in range(TOP // 2)]
        base = jnp.where(msg_row == 0, words[0], jnp.where(msg_row == 1, words[1], words[2]))
        for d in range(ndev):
            best = jnp.max(shifted[d * SLOT : (d + 1) * SLOT, :], axis=0, keepdims=True)
            code = (log_norm - best) * (LOG2E * MAX_SCALE) + 0.5
            code = jnp.clip(code, 0.0, 2.0e9).astype(jnp.int32)
            sent_msg[d, c] = jnp.where(msg_row == 3, code, base)
        recv_msg[me, c] = sent_msg[me, c]
        for j in range(1, ndev):
            message_copy(j, c).start()
        return carry

    lax.fori_loop(0, chunks, step, 0)

    pltpu.make_async_copy(cnt_recv.at[pl.ds(0, everyone - 1)], cnt_recv.at[pl.ds(0, everyone - 1)], cr_sem).wait()
    all_counts = jnp.sum(cnt_recv[...], axis=0)
    freq = jnp.zeros((nrows, 1), jnp.float32)
    dev_freq = jnp.zeros((nrows, 1), jnp.float32)
    sent = jnp.zeros((nrows, 1), jnp.float32)
    for p in range(pages):
        here = all_counts[:, p * 128 : (p + 1) * 128]
        there = all_counts[:, (pages + p) * 128 : (pages + p + 1) * 128]
        where = lane + p * 128
        same = (where // SLOT) == (row // SLOT)
        freq = freq + jnp.sum(jnp.where(where == row, here, nil), axis=1, keepdims=True)
        dev_freq = dev_freq + jnp.sum(jnp.where(same, here, nil), axis=1, keepdims=True)
        sent = sent + jnp.sum(jnp.where(same, there, nil), axis=1, keepdims=True)
    experts = ndev * per_dev
    freq = freq * (experts / (TOP * total))
    dev_freq = dev_freq * (experts / (TOP * total) / per_dev)
    sent = sent * (ndev / (DEV_TOP * total))
    prob = prob_acc[...] * (1.0 / total)
    one_lane = lax.broadcasted_iota(jnp.int32, (1, 128), 1)
    result = jnp.zeros((1, 128), jnp.float32)
    for i, factor in enumerate((freq, dev_freq, sent)):
        part = jnp.sum(jnp.sum(prob * factor, axis=0, keepdims=True), axis=1, keepdims=True)
        result = jnp.where(one_lane == i, part, result)
    bal_msg[...] = result
    bal_recv[lin] = result

    def bal_copy(j):
        return pltpu.make_async_remote_copy(
            src_ref=bal_msg, dst_ref=bal_recv.at[lin], send_sem=bs_sem, recv_sem=br_sem,
            device_id=other(j), device_id_type=MESH,
        )

    def start_bal(j, carry):
        bal_copy(j).start()
        return carry

    lax.fori_loop(1, everyone, start_bal, 0)

    def decode(src):
        def body(c, carry):
            words = recv_msg[src, c]
            low = jnp.exp2((words & 65535).astype(jnp.float32) * (-1.0 / GATE_SCALE))
            high = jnp.exp2(lax.shift_right_logical(words, 16).astype(jnp.float32) * (-1.0 / GATE_SCALE))
            top = jnp.exp2(words[3:4, :].astype(jnp.float32) * (-1.0 / MAX_SCALE))
            cols = pl.ds(pl.multiple_of(src * share + c * width, width), width)
            gates[0:3, cols] = low[0:3]
            gates[3:6, cols] = high[0:3]
            device_max[:, cols] = top
            return carry

        lax.fori_loop(0, chunks, body, 0)

    decode(me)
    for j in range(1, ndev):
        src = lax.rem(me + ndev - j, ndev)
        pltpu.make_async_copy(recv_msg.at[src], recv_msg.at[src], mr_sem.at[j]).wait()
        decode(src)

    pltpu.make_async_copy(bal_recv.at[pl.ds(0, everyone - 1)], bal_recv.at[pl.ds(0, everyone - 1)], br_sem).wait()
    sums = jnp.sum(bal_recv[...], axis=0)
    for i in range(3):
        balance[i] = jnp.sum(jnp.where(one_lane == i, sums, nil))

    for j in range(1, ndev):
        router_copy(j).wait_send()
        partner_copy(j).wait_send()
        peer = lax.rem(me + j, ndev)
        pltpu.make_async_copy(sent_msg.at[peer], sent_msg.at[peer], ms_sem.at[j]).wait()
    pltpu.make_async_copy(cnt_recv.at[pl.ds(0, everyone - 1)], cnt_recv.at[pl.ds(0, everyone - 1)], cs_sem).wait()
    pltpu.make_async_copy(bal_recv.at[pl.ds(0, everyone - 1)], bal_recv.at[pl.ds(0, everyone - 1)], bs_sem).wait()


def local(tokens, router, device_pick, expert_pick):
    depth, share = tokens.shape
    ndev, ndp = lax.axis_size("expert"), lax.axis_size("dp")
    per_dev = router.shape[1]
    width = min(512, share)
    chunks = share // width
    nrows = ndev * SLOT
    padded = (nrows + 127) // 128 * 128
    everyone = ndp * ndev
    router = jnp.pad(router.T, ((0, SLOT - per_dev), (0, 0)))
    dma = pltpu.SemaphoreType.DMA
    gates, device_max, balance = pl.pallas_call(
        functools.partial(kernel, (ndp, ndev, per_dev, width, chunks)),
        out_shape=(
            jax.ShapeDtypeStruct((TOP, share * ndev), jnp.float32),
            jax.ShapeDtypeStruct((1, share * ndev), jnp.float32),
            jax.ShapeDtypeStruct((3,), jnp.float32),
        ),
        in_specs=[
            pl.BlockSpec(memory_space=pl.ANY),
            pl.BlockSpec(memory_space=pltpu.VMEM),
            pl.BlockSpec(memory_space=pl.ANY),
            pl.BlockSpec(memory_space=pl.ANY),
        ],
        out_specs=(
            pl.BlockSpec(memory_space=pltpu.VMEM),
            pl.BlockSpec(memory_space=pltpu.VMEM),
            pl.BlockSpec(memory_space=pltpu.SMEM),
        ),
        scratch_shapes=[
            pltpu.VMEM((chunks, depth, width), jnp.bfloat16),
            pltpu.VMEM((nrows, depth), jnp.bfloat16),
            pltpu.VMEM((TOP, share), jnp.int32),
            pltpu.VMEM((DEV_TOP, share), jnp.int32),
            pltpu.VMEM((ndev, chunks, 4, width), jnp.int32),
            pltpu.VMEM((ndev, chunks, 4, width), jnp.int32),
            pltpu.VMEM((1, 2 * padded), jnp.float32),
            pltpu.VMEM((everyone, 1, 2 * padded), jnp.float32),
            pltpu.VMEM((1, 128), jnp.float32),
            pltpu.VMEM((everyone, 1, 128), jnp.float32),
            pltpu.VMEM((nrows, 128), jnp.float32),
            dma((chunks,)),
            dma((2,)),
            dma((ndev,)),
            dma((ndev,)),
            dma((ndev,)),
            dma((ndev,)),
            dma((ndev,)),
            dma((ndev,)),
            dma,
            dma,
            dma,
            dma,
        ],
        compiler_params=pltpu.CompilerParams(
            collective_id=0, has_side_effects=True, vmem_limit_bytes=60 * 1024 * 1024
        ),
        name="route",
    )(tokens, router, device_pick, expert_pick)
    return gates, device_max, balance


def solution(mesh):
    placed = (P(None, ("dp", "expert")), P(None, "expert"), P(None, "dp"), P(None, "dp"))
    return jax.shard_map(
        local,
        mesh=mesh,
        in_specs=placed,
        out_specs=(P(None, "dp"), P("expert", "dp"), P()),
        check_vma=False,
    )
```

```python
import functools

import jax
import jax.numpy as jnp
from jax import lax
from jax.experimental import pallas as pl
from jax.experimental.pallas import tpu as pltpu
from jax.sharding import PartitionSpec as P

MESH = pl.DeviceIdType.MESH
TOP = 6
DEV_TOP = 3
SLOT = 8
LOG2E = 1.4426950408889634
GATE_SCALE = 2048.0
NEG = -1e30
VMEM = 67043328


def kernel(
    sizes, tokens, router, device_pick, expert_pick,
    recv_msg, balance,
    tok, raw, own_rows, rows, picks, dpicks, sent_msg, cnt_msg, cnt_recv, bal_msg, bal_recv, prob_acc,
    tok_sem, pick_sem, rs_sem, rr_sem, ys_sem, yr_sem, ps_sem, pr_sem,
    ms_sem, mr_sem, fs_sem, fr_sem, cs_sem, cr_sem, bs_sem, br_sem,
):
    ndp, ndev, per_dev, width, chunks = sizes
    depth = tokens.shape[0]
    share = tokens.shape[1]
    total = share * ndev * ndp
    nrows = ndev * SLOT
    everyone = ndp * ndev
    half = depth // 2
    dp, me = lax.axis_index("dp"), lax.axis_index("expert")
    lin = dp * ndev + me
    core = lax.rem(dp, 2)
    partner = dp + 1 - 2 * core

    def token_copy(c):
        return pltpu.make_async_copy(
            tokens.at[:, pl.ds(pl.multiple_of(c * width, width), width)], tok.at[c], tok_sem.at[c]
        )

    mine = pl.ds(pl.multiple_of(me * share, share), share)
    pick_copy = pltpu.make_async_copy(expert_pick.at[:, mine], picks, pick_sem.at[0])
    dpick_copy = pltpu.make_async_copy(device_pick.at[:, mine], dpicks, pick_sem.at[1])
    raw_copy = pltpu.make_async_copy(router, raw, pick_sem.at[2])
    raw_copy.start()
    pick_copy.start()
    dpick_copy.start()
    for c in range(chunks):
        token_copy(c).start()

    barrier = pltpu.get_barrier_semaphore()

    def other(j):
        t = lax.rem(lin + j, everyone)
        return (t // ndev, lax.rem(t, ndev))

    def greet(j, carry):
        pl.semaphore_signal(barrier, inc=1, device_id=other(j), device_id_type=MESH)
        return carry

    lax.fori_loop(1, everyone, greet, 0)
    raw_copy.wait()
    pad = jnp.zeros((SLOT - per_dev, depth), jnp.float32)
    own_rows[...] = jnp.concatenate([raw[...].astype(jnp.float32), pad], axis=0).astype(jnp.bfloat16)
    pl.semaphore_wait(barrier, everyone - 1)

    pairs = ndev // 2
    my_pair, side = me // 2, lax.rem(me, 2)
    mate = me + 1 - 2 * side

    def ahead(j):
        return lax.rem(my_pair + j, pairs) * 2 + side

    def behind(j, which):
        return lax.rem(my_pair + pairs - j, pairs) * 2 + which

    my_half = pl.ds(pl.multiple_of(core * half, half), half)
    my_rows = pl.ds(pl.multiple_of(me * SLOT, SLOT), SLOT)

    def slot(src):
        return rows.at[pl.ds(pl.multiple_of(src * SLOT, SLOT), SLOT), my_half]

    def router_copy(j):
        return pltpu.make_async_remote_copy(
            src_ref=own_rows.at[:, my_half], dst_ref=slot(me),
            send_sem=rs_sem.at[j], recv_sem=rr_sem.at[j], device_id=(dp, ahead(j)), device_id_type=MESH,
        )

    def mate_copy(j):
        return pltpu.make_async_remote_copy(
            src_ref=own_rows.at[:, my_half] if j == 0 else slot(behind(j, side)), dst_ref=slot(behind(j, side)),
            send_sem=ys_sem.at[j], recv_sem=yr_sem.at[j], device_id=(dp, mate), device_id_type=MESH,
        )

    def partner_copy(j, other_side):
        block = slot(behind(j, 1 - side if other_side else side))
        spot = j + other_side * pairs
        return pltpu.make_async_remote_copy(
            src_ref=block, dst_ref=block, send_sem=ps_sem.at[spot], recv_sem=pr_sem.at[spot],
            device_id=(partner, me), device_id_type=MESH,
        )

    for j in range(1, pairs):
        router_copy(j).start()
    mate_copy(0).start()
    own = pltpu.make_async_copy(own_rows, rows.at[my_rows, :], rs_sem.at[0])
    own.start()

    pick_copy.wait()
    dpick_copy.wait()
    row = lax.broadcasted_iota(jnp.int32, (nrows, 128), 0)
    lane = lax.broadcasted_iota(jnp.int32, (nrows, 128), 1)
    one, nil = jnp.float32(1.0), jnp.float32(0.0)
    ids = (row // SLOT) * per_dev + lax.rem(row, SLOT)
    ids = jnp.where(lax.rem(row, SLOT) < per_dev, ids, -1)
    dev_ids = jnp.where(lax.rem(row, SLOT) == 0, row // SLOT, -1)

    def count(i, carry):
        counts, sends = carry
        cols = pl.ds(pl.multiple_of(i * 128, 128), 128)
        for k in range(TOP):
            counts = counts + jnp.where(picks[k : k + 1, cols] == ids, one, nil)
        for k in range(DEV_TOP):
            sends = sends + jnp.where(dpicks[k : k + 1, cols] == dev_ids, one, nil)
        return counts, sends

    zero = jnp.zeros((nrows, 128), jnp.float32)
    counts, sends = lax.fori_loop(0, share // 128, count, (zero, zero))
    counts = jnp.sum(counts, axis=1, keepdims=True)
    sends = jnp.sum(sends, axis=1, keepdims=True)
    pages = cnt_msg.shape[1] // 2 // 128
    for p in range(pages):
        spot = row == lane + p * 128
        cnt_msg[:, p * 128 : (p + 1) * 128] = jnp.sum(jnp.where(spot, counts, nil), axis=0, keepdims=True)
        cnt_msg[:, (pages + p) * 128 : (pages + p + 1) * 128] = jnp.sum(
            jnp.where(spot, sends, nil), axis=0, keepdims=True
        )
    cnt_recv[lin] = cnt_msg[...]

    def count_copy(j):
        return pltpu.make_async_remote_copy(
            src_ref=cnt_msg, dst_ref=cnt_recv.at[lin], send_sem=cs_sem, recv_sem=cr_sem,
            device_id=other(j), device_id_type=MESH,
        )

    def start_count(j, carry):
        count_copy(j).start()
        return carry

    lax.fori_loop(1, everyone, start_count, 0)

    own.wait()
    for j in range(1, pairs):
        router_copy(j).wait_recv()
        mate_copy(j).start()
        partner_copy(j, 0).start()
    for j in range(pairs):
        mate_copy(j).wait_recv()
        partner_copy(j, 1).start()
    for j in range(1, pairs):
        partner_copy(j, 0).wait_recv()
    for j in range(pairs):
        partner_copy(j, 1).wait_recv()

    prob_acc[...] = zero
    wide_row = lax.broadcasted_iota(jnp.int32, (nrows, width), 0)
    wide_ids = (wide_row // SLOT) * per_dev + lax.rem(wide_row, SLOT)
    real = lax.rem(wide_row, SLOT) < per_dev
    wide_ids = jnp.where(real, wide_ids, -1)
    msg_row = lax.broadcasted_iota(jnp.int32, (4, width), 0)

    def message_copy(j, c):
        return pltpu.make_async_remote_copy(
            src_ref=sent_msg.at[lax.rem(my_pair + j, pairs), c], dst_ref=recv_msg.at[me, c],
            send_sem=ms_sem.at[j], recv_sem=mr_sem.at[j, c], device_id=(dp, ahead(j)), device_id_type=MESH,
        )

    def forward_copy(j, c):
        src = behind(j, side)
        return pltpu.make_async_remote_copy(
            src_ref=sent_msg.at[my_pair, c] if j == 0 else recv_msg.at[src, c], dst_ref=recv_msg.at[src, c],
            send_sem=fs_sem.at[j], recv_sem=fr_sem.at[j], device_id=(dp, mate), device_id_type=MESH,
        )

    def forward(c):
        for j in range(1, pairs):
            message_copy(j, c).wait_recv()
            forward_copy(j, c).start()

    def step(c, carry):
        token_copy(c).wait()
        scores = jnp.dot(rows[...], tok[c], preferred_element_type=jnp.float32)
        scores = jnp.where(real, scores, NEG)
        peak = jnp.max(scores, axis=0, keepdims=True)
        shifted = scores - peak
        raised = jnp.exp(shifted)
        norm = jnp.sum(raised, axis=0, keepdims=True)
        probs = raised * (1.0 / norm)
        acc = prob_acc[...]
        for i in range(width // 128):
            acc = acc + probs[:, i * 128 : (i + 1) * 128]
        prob_acc[...] = acc
        log_norm = jnp.log(norm)
        cols = pl.ds(pl.multiple_of(c * width, width), width)
        codes = []
        for k in range(TOP):
            hit = picks[k : k + 1, cols] == wide_ids
            picked = jnp.sum(jnp.where(hit, shifted, nil), axis=0, keepdims=True)
            code = (log_norm - picked) * (LOG2E * GATE_SCALE) + 0.5
            codes.append(jnp.clip(code, 0.0, 65535.0).astype(jnp.int32))
        words = [codes[k] + jnp.left_shift(codes[k + TOP // 2], 16) for k in range(TOP // 2)]
        base = jnp.where(msg_row == 0, words[0], jnp.where(msg_row == 1, words[1], words[2]))
        tops = []
        for d in range(ndev):
            best = jnp.max(shifted[d * SLOT : (d + 1) * SLOT, :], axis=0, keepdims=True)
            code = (log_norm - best) * (LOG2E * GATE_SCALE) + 0.5
            tops.append(jnp.clip(code, 0.0, 65535.0).astype(jnp.int32))
        for p in range(pairs):
            top = tops[2 * p] + jnp.left_shift(tops[2 * p + 1], 16)
            sent_msg[p, c] = jnp.where(msg_row == 3, top, base)
        recv_msg[me, c] = sent_msg[my_pair, c]
        for j in range(1, pairs):
            message_copy(j, c).start()
        forward_copy(0, c).start()

        @pl.when(c >= lag)
        def _():
            forward(c - lag)

        return carry

    lag = min(3, chunks)
    lax.fori_loop(0, chunks, step, 0)

    pltpu.make_async_copy(cnt_recv.at[pl.ds(0, everyone - 1)], cnt_recv.at[pl.ds(0, everyone - 1)], cr_sem).wait()
    all_counts = jnp.sum(cnt_recv[...], axis=0)
    freq = jnp.zeros((nrows, 1), jnp.float32)
    dev_freq = jnp.zeros((nrows, 1), jnp.float32)
    sent = jnp.zeros((nrows, 1), jnp.float32)
    for p in range(pages):
        here = all_counts[:, p * 128 : (p + 1) * 128]
        there = all_counts[:, (pages + p) * 128 : (pages + p + 1) * 128]
        where = lane + p * 128
        same = (where // SLOT) == (row // SLOT)
        freq = freq + jnp.sum(jnp.where(where == row, here, nil), axis=1, keepdims=True)
        dev_freq = dev_freq + jnp.sum(jnp.where(same, here, nil), axis=1, keepdims=True)
        sent = sent + jnp.sum(jnp.where(same, there, nil), axis=1, keepdims=True)
    experts = ndev * per_dev
    freq = freq * (experts / (TOP * total))
    dev_freq = dev_freq * (experts / (TOP * total) / per_dev)
    sent = sent * (ndev / (DEV_TOP * total))
    prob = prob_acc[...] * (1.0 / total)
    one_lane = lax.broadcasted_iota(jnp.int32, (1, 128), 1)
    result = jnp.zeros((1, 128), jnp.float32)
    for i, factor in enumerate((freq, dev_freq, sent)):
        part = jnp.sum(jnp.sum(prob * factor, axis=0, keepdims=True), axis=1, keepdims=True)
        result = jnp.where(one_lane == i, part, result)
    bal_msg[...] = result
    bal_recv[lin] = result

    def bal_copy(j):
        return pltpu.make_async_remote_copy(
            src_ref=bal_msg, dst_ref=bal_recv.at[lin], send_sem=bs_sem, recv_sem=br_sem,
            device_id=other(j), device_id_type=MESH,
        )

    def start_bal(j, carry):
        bal_copy(j).start()
        return carry

    lax.fori_loop(1, everyone, start_bal, 0)

    for c in range(chunks - lag, chunks):
        forward(c)
    for j in range(pairs):
        src = behind(j, 1 - side)
        pltpu.make_async_copy(recv_msg.at[src], recv_msg.at[src], fr_sem.at[j]).wait()

    pltpu.make_async_copy(bal_recv.at[pl.ds(0, everyone - 1)], bal_recv.at[pl.ds(0, everyone - 1)], br_sem).wait()
    balance[...] = jnp.sum(bal_recv[...], axis=0)

    for j in range(pairs):
        if j:
            router_copy(j).wait_send()
            partner_copy(j, 0).wait_send()
            pltpu.make_async_copy(sent_msg.at[0], sent_msg.at[0], ms_sem.at[j]).wait()
        mate_copy(j).wait_send()
        partner_copy(j, 1).wait_send()
        pltpu.make_async_copy(sent_msg.at[0], sent_msg.at[0], fs_sem.at[j]).wait()
    pltpu.make_async_copy(cnt_recv.at[pl.ds(0, everyone - 1)], cnt_recv.at[pl.ds(0, everyone - 1)], cs_sem).wait()
    pltpu.make_async_copy(bal_recv.at[pl.ds(0, everyone - 1)], bal_recv.at[pl.ds(0, everyone - 1)], bs_sem).wait()


def decode(sizes, recv_msg, sums, gates, device_max, balance, gate_buf, top_buf, sem):
    ndev, share, width, chunks = sizes
    side = lax.rem(lax.axis_index("expert"), 2)
    copies = []
    for src in range(ndev):
        block = pl.ds(src * share, share)

        def body(c, carry):
            words = recv_msg[src, c]
            low = jnp.exp2((words & 65535).astype(jnp.float32) * (-1.0 / GATE_SCALE))
            high = jnp.exp2(lax.shift_right_logical(words, 16).astype(jnp.float32) * (-1.0 / GATE_SCALE))
            cols = pl.ds(pl.multiple_of(src * share + c * width, width), width)
            gate_buf[0:3, cols] = low[0:3]
            gate_buf[3:6, cols] = high[0:3]
            top_buf[:, cols] = jnp.where(side == 0, low[3:4], high[3:4])
            return carry

        lax.fori_loop(0, chunks, body, 0)
        copies.append(pltpu.make_async_copy(gate_buf.at[:, block], gates.at[:, block], sem.at[0, src]))
        copies.append(pltpu.make_async_copy(top_buf.at[:, block], device_max.at[:, block], sem.at[1, src]))
        copies[-2].start()
        copies[-1].start()
    lane = lax.broadcasted_iota(jnp.int32, (1, 128), 1)
    for i in range(3):
        balance[i] = jnp.sum(jnp.where(lane == i, sums[...], jnp.float32(0.0)))
    for copy in copies:
        copy.wait()


def local(tokens, router, device_pick, expert_pick):
    depth, share = tokens.shape
    ndev, ndp = lax.axis_size("expert"), lax.axis_size("dp")
    per_dev = router.shape[1]
    width = min(512, share)
    chunks = share // width
    nrows = ndev * SLOT
    padded = (nrows + 127) // 128 * 128
    everyone = ndp * ndev
    pairs = ndev // 2
    dma = pltpu.SemaphoreType.DMA
    messages, sums = pl.pallas_call(
        functools.partial(kernel, (ndp, ndev, per_dev, width, chunks)),
        out_shape=(
            jax.ShapeDtypeStruct((ndev, chunks, 4, width), jnp.int32),
            jax.ShapeDtypeStruct((1, 128), jnp.float32),
        ),
        in_specs=[pl.BlockSpec(memory_space=pltpu.HBM)] * 4,
        out_specs=(pl.BlockSpec(memory_space=pltpu.VMEM), pl.BlockSpec(memory_space=pltpu.VMEM)),
        scratch_shapes=[
            pltpu.VMEM((chunks, depth, width), jnp.bfloat16),
            pltpu.VMEM((per_dev, depth), jnp.bfloat16),
            pltpu.VMEM((SLOT, depth), jnp.bfloat16),
            pltpu.VMEM((nrows, depth), jnp.bfloat16),
            pltpu.VMEM((TOP, share), jnp.int32),
            pltpu.VMEM((DEV_TOP, share), jnp.int32),
            pltpu.VMEM((pairs, chunks, 4, width), jnp.int32),
            pltpu.VMEM((1, 2 * padded), jnp.float32),
            pltpu.VMEM((everyone, 1, 2 * padded), jnp.float32),
            pltpu.VMEM((1, 128), jnp.float32),
            pltpu.VMEM((everyone, 1, 128), jnp.float32),
            pltpu.VMEM((nrows, 128), jnp.float32),
            dma((chunks,)),
            dma((3,)),
            dma((pairs,)),
            dma((pairs,)),
            dma((pairs,)),
            dma((pairs,)),
            dma((2 * pairs,)),
            dma((2 * pairs,)),
            dma((pairs,)),
            dma((pairs, chunks)),
            dma((pairs,)),
            dma((pairs,)),
            dma,
            dma,
            dma,
            dma,
        ],
        compiler_params=pltpu.CompilerParams(
            collective_id=0, has_side_effects=True, vmem_limit_bytes=VMEM - share * ndev * 16 - 10747904
        ),
        name="route",
    )(tokens, router.T, device_pick, expert_pick)
    gates, device_max, balance = pl.pallas_call(
        functools.partial(decode, (ndev, share, width, chunks)),
        out_shape=(
            jax.ShapeDtypeStruct((TOP, share * ndev), jnp.float32),
            jax.ShapeDtypeStruct((1, share * ndev), jnp.float32),
            jax.ShapeDtypeStruct((3,), jnp.float32),
        ),
        in_specs=[pl.BlockSpec(memory_space=pltpu.VMEM)] * 2,
        out_specs=(
            pl.BlockSpec(memory_space=pl.ANY),
            pl.BlockSpec(memory_space=pl.ANY),
            pl.BlockSpec(memory_space=pltpu.SMEM),
        ),
        scratch_shapes=[
            pltpu.VMEM((TOP, share * ndev), jnp.float32),
            pltpu.VMEM((1, share * ndev), jnp.float32),
            dma((2, ndev)),
        ],
        compiler_params=pltpu.CompilerParams(vmem_limit_bytes=8 * 1024 * 1024),
        name="decode",
    )(messages, sums)
    return gates, device_max, balance


def solution(mesh):
    placed = (P(None, ("dp", "expert")), P(None, "expert"), P(None, "dp"), P(None, "dp"))
    return jax.shard_map(
        local,
        mesh=mesh,
        in_specs=placed,
        out_specs=(P(None, "dp"), P("expert", "dp"), P()),
        check_vma=False,
    )
```
